256 devices in a mesh: rep: 32 (over y_lo, z, core), tp: 8 (over y_hi, x).
Axes of the slice: x: 4, y: 4 (y_hi: 2, y_lo: 2; y = y_hi * 2 + y_lo), z: 8, core: 2. Of those that a mesh axis runs over, the one named last changes fastest.
Arguments:
- positions: int32 [8192], P('rep'), may hold values from 0 to 8191
- activations: bfloat16 [8192, 4096], P('rep', 'tp'), may hold values from -6 to 6
- norm_gain: bfloat16 [4096], P('tp'), may hold values from 0.5 to 1.5
- qkv_weight: bfloat16 [4096, 6144], P('rep', 'tp'), may hold values from -0.09375 to 0.09375
- gate_up_weight: bfloat16 [4096, 14336], P('rep', 'tp'), may hold values from -0.09375 to 0.09375
Outputs:
- qkv_out: bfloat16 [8192, 6144], P('rep', 'tp')
- hidden: bfloat16 [8192, 7168], P('rep', 'tp')
The draws below stay inside these ranges and needn't reach their ends.
All inputs are finite; a program needn't handle non-finite values.
Results may differ from the reference program's by a relative error of at most 0.0058.
Values may be sent and summed in bfloat16 or wider, within the bound.
A program may use at most 128 MiB of HBM per device.

```python
import jax
import jax.numpy as jnp
from jax import lax

D = 4096
QH = 32
KVH = 8
HD = 128
FF = 7168
QKV = 6144
TOTAL_SEQS = 8192
N_TP = 8


def with_ends(entries, rng, smallest, largest):
    shape = entries.shape
    index_at = [jax.random.randint(jax.random.fold_in(rng, axis), (), 0, shape[axis]) for axis in range(len(shape))]
    entries = entries.at[tuple(index_at)].set(smallest)
    longest = shape.index(max(shape))
    index_at[longest] = (index_at[longest] + 1) % shape[longest]
    return entries.at[tuple(index_at)].set(largest)


def steps_of(rng, extent, pieces, low, largest):
    def one(axis_at, shards_of):
        heights = jax.random.uniform(jax.random.fold_in(jax.random.fold_in(rng, 6), axis_at), (shards_of,), jnp.float32, low / len(pieces), largest / len(pieces))
        return jnp.repeat(jnp.exp(heights), extent[axis_at] // shards_of).reshape((-1,) + (1,) * (len(extent) - axis_at - 1))

    loudness = one(*pieces[0])
    for cut in pieces[1:]:
        loudness = loudness * one(*cut)
    return loudness


def gaussian(key, shape, scale, most, pieces=(), kind=jnp.bfloat16):
    entries = scale * jax.random.normal(key, shape, jnp.float32)
    if pieces:
        entries = entries * steps_of(key, shape, pieces, -0.22, 0.18)
    return jnp.clip(entries, -most, most).astype(kind)


def setup_inputs(seed: int = 0) -> dict:
    seeds = jax.random.split(jax.random.key(seed), 6)
    return {
        "positions": with_ends(jax.random.randint(seeds[0], (TOTAL_SEQS,), 0, 8192), jax.random.fold_in(seeds[0], 1), 0, 8191).astype(jnp.int32),
        "activations": gaussian(seeds[1], (TOTAL_SEQS, D), 1.0, 6.0, ((0, 32), (1, 8))),
        "norm_gain": jnp.clip(1.0 + 0.1 * jax.random.normal(seeds[2], (D,), jnp.float32), 0.5, 1.5).astype(jnp.bfloat16),
        "qkv_weight": gaussian(seeds[3], (D, QKV), D ** -0.5, 0.09375, ((0, 32), (1, 8))),
        "gate_up_weight": gaussian(seeds[4], (D, 2 * FF), D ** -0.5, 0.09375, ((0, 32), (1, 8))),
    }


theta_base = 500000.0
norm_eps = 1e-05

def normalize(gathered, gain_row):
    values = gathered.astype(jnp.float32)
    mean_square = lax.optimization_barrier(jnp.mean(values * values, axis=1, keepdims=True))
    return (values * lax.rsqrt(mean_square + norm_eps) * gain_row.astype(jnp.float32)).astype(jnp.bfloat16)

def rotary(joined_qkv, positions):
    row_count = joined_qkv.shape[0]
    per_group = QH // KVH + 2
    half_size = HD // 2
    head_view = joined_qkv.reshape(row_count, -1, per_group, HD)
    frequency = theta_base ** (-2.0 * jnp.arange(half_size, dtype=jnp.float32) / HD)
    angles = positions.astype(jnp.float32)[:, None] * frequency[None, :]
    cosine = jnp.cos(angles)[:, None, None, :]
    sine_part = jnp.sin(angles)[:, None, None, :]
    leading = head_view[..., :half_size]
    trailing = head_view[..., half_size:]
    turned = jnp.concatenate([leading * cosine - trailing * sine_part, trailing * cosine + leading * sine_part], axis=-1)
    rotated_mask = (jnp.arange(per_group) < per_group - 1)[None, None, :, None]
    return jnp.where(rotated_mask, turned, head_view).reshape(row_count, -1)

def reference(positions, activations, norm_gain, qkv_weight, gate_up_weight):
    normed = normalize(activations, norm_gain)
    joined_qkv = jnp.dot(normed, qkv_weight, preferred_element_type=jnp.float32)
    qkv_out = rotary(joined_qkv, positions).astype(jnp.bfloat16)
    gate_up = jnp.dot(normed, gate_up_weight, preferred_element_type=jnp.float32)
    row_count = gate_up.shape[0]
    paired = gate_up.reshape(row_count, N_TP, 2, FF // N_TP)
    hidden = (jax.nn.silu(paired[:, :, 0]) * paired[:, :, 1]).reshape(row_count, FF).astype(jnp.bfloat16)
    return (qkv_out, hidden)
```

```python
import jax
import jax.numpy as jnp
from jax import lax
from jax.experimental import pallas as pl
from jax.experimental.pallas import tpu as pltpu
from jax.sharding import PartitionSpec as P

HD = 128
theta_base = 500000.0
norm_eps = 1e-05

MESH = pl.DeviceIdType.MESH
NB = 5
FIRST = 3
OFF = (0, 3, 1, 2)
COLORS = (("x", "y", 1), ("x", "y", -1), ("y", "x", 1), ("y", "x", -1), ("x", "y", 1))


def kernel(
    cs_ref, x_ref, g_ref, wq_ref, wg_ref, oq_ref, oh_ref,
    S, W, A, G, N, T, ACC, OS,
    ld_sem, z_send, z_recv, d_send, d_recv, ye_send, ye_recv,
    a_send, a_recv, t_sem, o_send, o_recv, o_loc,
):
    rep = lax.axis_index("rep")
    tp = lax.axis_index("tp")
    core = rep % 2
    z = (rep // 2) % 8
    yl = rep // 16
    x = tp % 4
    y = (tp // 4) * 2 + yl

    def dev(xx, yy, zz, cc):
        return (((yy % 2) * 8 + zz) * 2 + cc, (yy // 2) * 4 + xx)

    xp, xm = dev((x + 1) % 4, y, z, core), dev((x + 3) % 4, y, z, core)
    yp, ym = dev(x, (y + 1) % 4, z, core), dev(x, (y + 3) % 4, z, core)
    zp, zm = dev(x, y, (z + 1) % 8, core), dev(x, y, (z + 7) % 8, core)
    pc = dev(x, y, z, 1 - core)
    yo = (((1 - yl) * 8 + z) * 2 + core, tp)
    step_to = {("x", 1): xp, ("x", -1): xm, ("y", 1): yp, ("y", -1): ym}

    barrier = pltpu.get_barrier_semaphore()
    for d in (xp, xm, yp, ym, zp, zm, pc):
        pl.semaphore_signal(barrier, inc=1, device_id=d, device_id_type=MESH)

    act_load = pltpu.make_async_copy(x_ref, A.at[tp, pl.ds(yl * 256, 256), :], ld_sem.at[1])
    act_load.start()
    gain_load = pltpu.make_async_copy(g_ref, G.at[tp, yl], ld_sem.at[2])
    gain_load.start()
    for s, c in ((0, 0), (5, 256), (6, 512)):
        pltpu.make_async_copy(wq_ref.at[:, pl.ds(c, 256)], S.at[s], ld_sem.at[0]).start()
    for p in range(7):
        s = p + 1 if p < 4 else p + 3
        for side in range(2):
            pltpu.make_async_copy(
                wg_ref.at[:, pl.ds(side * 896 + p * 128, 128)],
                S.at[s, :, pl.ds(side * 128, 128)],
                ld_sem.at[0],
            ).start()
    t_load = pltpu.make_async_copy(cs_ref, T.at[yl], ld_sem.at[3])
    t_load.start()

    def remote(src, dst, ssem, rsem, to):
        return pltpu.make_async_remote_copy(
            src_ref=src, dst_ref=dst, send_sem=ssem, recv_sem=rsem, device_id=to, device_id_type=MESH
        )

    def w_at(b, py, pz, pcore):
        return W.at[b, py * 8 + pz, pl.ds(pcore * 128, 128), :]

    def plane(s):
        return yl if s == 0 else 1 - yl

    def z_copy(b, s, dr, h, own=False):
        src_z = (z - dr * (h - 1) + 8) % 8
        ref = w_at(b, plane(s), src_z, core)
        src = S.at[yl * NB + b] if own else ref
        i = (((0 if dr == 1 else 1) * 4 + (h - 1)) * 2 + s) * NB + b
        return remote(src, ref, z_send.at[i], z_recv.at[i], zp if dr == 1 else zm)

    def z_wait(b, s, dr, h):
        src_z = (z - dr * h + 8) % 8
        ref = w_at(b, plane(s), src_z, core)
        i = (((0 if dr == 1 else 1) * 4 + (h - 1)) * 2 + s) * NB + b
        remote(ref, ref, z_send.at[i], z_recv.at[i], zp if dr == 1 else zm).wait_recv()

    def d_copy(b, s, j, own=False):
        src_z = (z + j + 8) % 8
        ref = w_at(b, plane(s), src_z, core)
        src = S.at[yl * NB + b] if own else ref
        i = ((j + 3) * 2 + s) * NB + b
        return remote(src, ref, d_send.at[i], d_recv.at[i], pc)

    def d_wait(b, s, j):
        src_z = (z + j + 8) % 8
        ref = w_at(b, plane(s), src_z, 1 - core)
        i = ((j + 3) * 2 + s) * NB + b
        remote(ref, ref, d_send.at[i], d_recv.at[i], pc).wait_recv()

    def a_at(c, o1, o2):
        ox, oy = (o1, o2) if COLORS[c][0] == "x" else (o2, o1)
        xx = (x + OFF[ox]) % 4
        yy = (y + OFF[oy]) % 4
        t = (yy // 2) * 4 + xx
        if c == 4:
            return G.at[t, yy % 2]
        return A.at[t, pl.ds((yy % 2) * 256 + c * 64, 64), :]

    def a_send_to(c, phase, o1, o2, sign, kind):
        r1, r2 = (kind, o2) if phase == 0 else (o1, kind)
        ref = a_at(c, o1, o2)
        i = c * 16 + r1 * 4 + r2
        return remote(ref, ref, a_send.at[i], a_recv.at[i], step_to[(COLORS[c][phase], sign)])

    def a_both(c, phase, o1, o2):
        a_send_to(c, phase, o1, o2, 1, 1).start()
        a_send_to(c, phase, o1, o2, -1, 2).start()

    def a_relay(c, phase, o1, o2):
        a_send_to(c, phase, o1, o2, COLORS[c][2], 3).start()

    def a_wait(c, o1, o2):
        ref = a_at(c, o1, o2)
        i = c * 16 + o1 * 4 + o2
        remote(ref, ref, a_send.at[i], a_recv.at[i], xp).wait_recv()

    def long_kind(c):
        return 1 if COLORS[c][2] == 1 else 2

    def short_kind(c):
        return 2 if COLORS[c][2] == 1 else 1

    def blocks(lo, hi, f):
        def body(b, carry):
            f(b)
            return carry

        lax.fori_loop(lo, hi, body, 0)

    act_load.wait()
    gain_load.wait()
    pl.semaphore_wait(barrier, 7)

    for c in (2, 3, 0, 1, 4):
        a_both(c, 0, 0, 0)
    pltpu.make_async_copy(S, S, ld_sem.at[0]).wait()

    def start_own(b):
        z_copy(b, 0, 1, 1, own=True).start()
        z_copy(b, 0, -1, 1, own=True).start()
        remote(
            S.at[(1 - yl) * NB + b], w_at(b, yl, z, core), ye_send.at[b], ye_recv.at[b], yo
        ).start()
        d_copy(b, 0, 0, own=True).start()

    blocks(0, NB, start_own)
    for c in (0, 1, 4, 2, 3):
        a_both(c, 1, 0, 0)

    def keep_own(b):
        W[b, yl * 8 + z, pl.ds(core * 128, 128), :] = S[yl * NB + b]

    blocks(0, NB, keep_own)

    for c in (2, 3, 0, 1, 4):
        o = long_kind(c)
        a_wait(c, o, 0)
        a_relay(c, 0, o, 0)
        a_both(c, 1, o, 0)
    for c in (2, 3, 0, 1, 4):
        o = short_kind(c)
        a_wait(c, o, 0)
        a_both(c, 1, o, 0)

    def start_other(b):
        ref = w_at(b, 1 - yl, z, core)
        remote(ref, ref, ye_send.at[b], ye_recv.at[b], yo).wait_recv()
        z_copy(b, 1, 1, 1).start()
        z_copy(b, 1, -1, 1).start()
        d_copy(b, 1, 0).start()

    blocks(0, NB, start_other)

    for c in (2, 3, 0, 1, 4):
        a_wait(c, 3, 0)
        a_both(c, 1, 3, 0)

    def arrive(h, s, forward):
        def f(b):
            for dr in (1, -1):
                if h == 4 and (dr == 1) != (s == 0):
                    continue
                z_wait(b, s, dr, h)
                if forward and not (h == 3 and (dr == 1) != (s == 0)):
                    z_copy(b, s, dr, h + 1).start()
                d_copy(b, s, 4 if h == 4 else -dr * h).start()

        return f

    def second_relays(o1):
        for c in (0, 1, 2, 3, 4):
            a_wait(c, o1, long_kind(c))
            a_relay(c, 1, o1, long_kind(c))

    blocks(0, FIRST, arrive(1, 0, True))
    second_relays(0)
    blocks(0, FIRST, arrive(1, 1, True))
    for o1 in (1, 2):
        second_relays(o1)
    blocks(FIRST, NB, arrive(1, 0, False))
    blocks(FIRST, NB, arrive(1, 1, False))
    second_relays(3)
    blocks(0, FIRST, arrive(2, 0, True))
    blocks(0, FIRST, arrive(2, 1, True))
    t_load.wait()
    t_copy = remote(T.at[yl], T.at[yl], t_sem.at[0], t_sem.at[1], yo)
    t_copy.start()
    blocks(0, FIRST, arrive(3, 0, True))
    for o1 in (0, 1, 2, 3):
        for c in (0, 1, 2, 3, 4):
            a_wait(c, o1, short_kind(c))
            a_wait(c, o1, 3)

    def norm_rows(i, carry):
        rows = pl.ds(i * 32, 32)
        total = jnp.zeros((32, 128), jnp.float32)
        for t in range(8):
            v = A[t, rows, :].astype(jnp.float32)
            v = v * v
            total = total + ((v[:, 0:128] + v[:, 128:256]) + (v[:, 256:384] + v[:, 384:512]))
        mean_square = jnp.sum(total, axis=1, keepdims=True) * (1.0 / 4096.0)
        scale = lax.rsqrt(mean_square + norm_eps)
        for t in range(8):
            v = A[t, rows, :].astype(jnp.float32)
            g = G[t, 0].astype(jnp.float32)
            v = (v * scale * g).astype(jnp.bfloat16)
            N[2 * t, rows, :] = v[:, 0:256]
            N[2 * t + 1, rows, :] = v[:, 256:512]
        return carry

    lax.fori_loop(0, 16, norm_rows, 0)

    blocks(0, FIRST, arrive(3, 1, True))

    def forward_second(s):
        def f(b):
            z_copy(b, s, 1, 2).start()
            z_copy(b, s, -1, 2).start()

        return f

    for s in range(2):
        blocks(FIRST, NB, forward_second(s))

    def compute(js, first):
        def f(b):
            for j in js:
                for s in range(2):
                    d_wait(b, s, j)

            def body(m, carry):
                rows = pl.ds(m * 256, 256)
                total = None if first else ACC[b, rows, :]
                for j in js:
                    zz = (z + j + 8) % 8
                    for half in range(2):
                        k = half * 8 + zz
                        part = jnp.dot(N[k, rows, :], W[b, k], preferred_element_type=jnp.float32)
                        total = part if total is None else total + part
                ACC[b, rows, :] = total
                return carry

            lax.fori_loop(0, 2, body, 0)

        return f

    lane = lax.broadcasted_iota(jnp.int32, (32, 128), 1)

    def pair_rows(b):
        def body(i, carry):
            rows = pl.ds(i * 32, 32)
            gate = ACC[b, rows, 0:128]
            up = ACC[b, rows, 128:256]
            OS[b, rows, 0:128] = (gate / (1.0 + jnp.exp(-gate)) * up).astype(jnp.bfloat16)
            return carry

        lax.fori_loop(0, 16, body, 0)

    def head_rows(b):
        def body(i, carry):
            rows = pl.ds(i * 32, 32)
            table = T[i // 8, pl.ds((i % 8) * 32, 32), :]
            turned = pltpu.roll(table, 64, 1)
            cosine = jnp.where(lane < 64, table, turned)
            sine = jnp.where(lane < 64, -turned, table)
            for head in range(2):
                v = ACC[b, rows, pl.ds(head * 128, 128)]
                r = v * cosine + pltpu.roll(v, 64, 1) * sine
                if b == 1 and head == 1:
                    r = v
                OS[b, rows, pl.ds(head * 128, 128)] = r.astype(jnp.bfloat16)
            return carry

        lax.fori_loop(0, 16, body, 0)

    def is_head(b, half, then, other):
        if b == 0:
            then()
        elif b == 1:
            pl.when(half == 1)(then)
            pl.when(half == 0)(other)
        else:
            other()

    def out_slices(b, half, head):
        if head:
            at = oq_ref.at[:, pl.ds(pl.multiple_of(256 * (b + half), 256), 256)]
        else:
            at = oh_ref.at[:, pl.ds(pl.multiple_of(128 * (b - 1 + 3 * half), 128), 128)]
        return at, 256 if head else 128

    def out_copies(b, head):
        at, width = out_slices(b, yl, head)
        away = remote(
            OS.at[b, pl.ds((1 - yl) * 256, 256), pl.ds(0, width)], at, o_send.at[b], o_recv.at[b], yo
        )
        here = pltpu.make_async_copy(OS.at[b, pl.ds(yl * 256, 256), pl.ds(0, width)], at, o_loc.at[b])
        return away, here

    def finish(b):
        def go(head):
            def f():
                (head_rows if head else pair_rows)(b)
                away, here = out_copies(b, head)
                away.start()
                here.start()

            return f

        is_head(b, yl, go(True), go(False))

    blocks(0, FIRST, compute((0, -1, 1, -2, 2), True))
    for s in range(2):
        blocks(0, FIRST, arrive(4, s, False))
    blocks(FIRST, NB, arrive(2, 0, True))
    blocks(0, FIRST, compute((-3, 3, 4), False))
    blocks(FIRST, NB, arrive(2, 1, True))
    remote(T.at[1 - yl], T.at[1 - yl], t_sem.at[0], t_sem.at[1], yo).wait_recv()
    for b in range(FIRST):
        finish(b)
    blocks(FIRST, NB, compute((0, -1, 1, -2, 2), True))
    for s in range(2):
        blocks(FIRST, NB, arrive(3, s, True))
    blocks(FIRST, NB, compute((-3, 3), False))
    for s in range(2):
        blocks(FIRST, NB, arrive(4, s, False))
    for b in range(FIRST, NB):
        compute((4,), False)(b)
        finish(b)

    t_copy.wait_send()

    def sent(b):
        ref = S.at[b]
        for s in range(2):
            for dr in range(2):
                for h in range(4):
                    if h == 3 and dr != s:
                        continue
                    i = ((dr * 4 + h) * 2 + s) * NB + b
                    remote(ref, ref, z_send.at[i], z_recv.at[i], zp).wait_send()
            for j in range(8):
                i = (j * 2 + s) * NB + b
                remote(ref, ref, d_send.at[i], d_recv.at[i], pc).wait_send()
        remote(ref, ref, ye_send.at[b], ye_recv.at[b], yo).wait_send()

    blocks(0, NB, sent)
    for c in range(5):
        for o1 in range(4):
            for o2 in range(4):
                if o1 or o2:
                    ref = a_at(c, 0, 0)
                    i = c * 16 + o1 * 4 + o2
                    remote(ref, ref, a_send.at[i], a_recv.at[i], xp).wait_send()

    for b in range(NB):

        def out_sent(head):
            def f():
                away, here = out_copies(b, head)
                here.wait()
                away.wait_send()

            return f

        is_head(b, yl, out_sent(True), out_sent(False))

        def out_arrived(head):
            def f():
                at, _ = out_slices(b, 1 - yl, head)
                remote(at, at, o_send.at[b], o_recv.at[b], yo).wait_recv()

            return f

        is_head(b, 1 - yl, out_arrived(True), out_arrived(False))


def per_device(positions, activations, norm_gain, qkv_weight, gate_up_weight):
    half_size = HD // 2
    frequency = theta_base ** (-2.0 * jnp.arange(half_size, dtype=jnp.float32) / HD)
    angles = positions.astype(jnp.float32)[:, None] * frequency[None, :]
    table = jnp.concatenate([jnp.cos(angles), jnp.sin(angles)], axis=1)
    sems = pltpu.SemaphoreType.DMA
    return pl.pallas_call(
        kernel,
        out_shape=(
            jax.ShapeDtypeStruct((256, 768), jnp.bfloat16),
            jax.ShapeDtypeStruct((256, 896), jnp.bfloat16),
        ),
        in_specs=[pl.BlockSpec(memory_space=pl.ANY)] * 5,
        out_specs=(pl.BlockSpec(memory_space=pl.ANY),) * 2,
        scratch_shapes=[
            pltpu.VMEM((2 * NB, 128, 256), jnp.bfloat16),
            pltpu.VMEM((NB, 16, 256, 256), jnp.bfloat16),
            pltpu.VMEM((8, 512, 512), jnp.bfloat16),
            pltpu.VMEM((8, 2, 1, 512), jnp.bfloat16),
            pltpu.VMEM((16, 512, 256), jnp.bfloat16),
            pltpu.VMEM((2, 256, 128), jnp.float32),
            pltpu.VMEM((NB, 512, 256), jnp.float32),
            pltpu.VMEM((NB, 512, 256), jnp.bfloat16),
            sems((4,)),
            sems((16 * NB,)),
            sems((16 * NB,)),
            sems((16 * NB,)),
            sems((16 * NB,)),
            sems((NB,)),
            sems((NB,)),
            sems((80,)),
            sems((80,)),
            sems((2,)),
            sems((NB,)),
            sems((NB,)),
            sems((NB,)),
        ],
        compiler_params=pltpu.CompilerParams(
            collective_id=0, has_side_effects=True, vmem_limit_bytes=48 * 1024 * 1024
        ),
    )(table, activations, norm_gain.reshape(1, 512), qkv_weight, gate_up_weight)


def solution(mesh):
    placed = (P("rep"), P("rep", "tp"), P("tp"), P("rep", "tp"), P("rep", "tp"))
    return jax.shard_map(
        per_device,
        mesh=mesh,
        in_specs=placed,
        out_specs=(P("rep", "tp"), P("rep", "tp")),
        check_vma=False,
    )
```
